32 devices in a mesh: rep: 1 (over z), fsdp: 4 (over y), ep: 8 (over x, core).
Axes of the slice: x: 4, y: 4, z: 1, core: 2. Of those that a mesh axis runs over, the one named last changes fastest.
The devices are a block of a 4x4x8 slice.
Arguments:
- tokens: bfloat16 [16384, 1536], P(('rep', 'ep', 'fsdp'))
- expert_idx: int32 [16384, 8], P(('rep', 'ep', 'fsdp'))
- gates: float32 [16384, 8], P(('rep', 'ep', 'fsdp'))
- w_gate: bfloat16 [40, 1536, 512], P('ep', 'fsdp')
- w_up: bfloat16 [40, 1536, 512], P('ep', 'fsdp')
- w_down: bfloat16 [40, 512, 1536], P('ep', None, 'fsdp')
Outputs:
- output: bfloat16 [16384, 1536], P(('rep', 'ep', 'fsdp'))
All inputs are finite; a program needn't handle non-finite values.
Results may differ from the reference program's by a relative error of at most 0.001.
Values are sent between devices in bfloat16 or wider.
A program may use at most 768 MiB of HBM per device.

```python
import jax
import jax.numpy as jnp
from jax import lax

TOK_DEV = 512
MODEL_DIM = 1536
FFN_DIM = 512
NUM_EXPERTS = 40
TOP_K = 8
EP_SIZE = 8
FSDP_SIZE = 4

GROUP_DEVS = EP_SIZE * FSDP_SIZE
ROW_COUNT = GROUP_DEVS * TOK_DEV
CAPACITY = (2 * TOK_DEV * TOP_K + NUM_EXPERTS - 1) // NUM_EXPERTS


def route_draw(key):
    key_rank, key_noise = jax.random.split(key)
    ranks = jax.random.permutation(key_rank, NUM_EXPERTS)
    skew = (ranks * 768) // NUM_EXPERTS
    noise = jax.random.randint(key_noise, (ROW_COUNT, NUM_EXPERTS), 0, 1024)
    scores = (noise + skew[None, :]) * NUM_EXPERTS + jnp.arange(NUM_EXPERTS)[None, :]
    top_vals, chosen = lax.top_k(scores, TOP_K)
    return chosen.astype(jnp.int32)


def setup_inputs(seed: int = 0, part: int = 0) -> dict:
    part_key = jax.random.fold_in(jax.random.key(seed), part)
    key_tok, key_route, key_gate = jax.random.split(part_key, 3)
    key_wg, key_wu, key_wd = jax.random.split(jax.random.key(seed + 1), 3)
    tokens = jax.random.normal(key_tok, (ROW_COUNT, MODEL_DIM), jnp.float32).astype(jnp.bfloat16)
    expert_idx = route_draw(key_route)
    gates = jax.random.uniform(key_gate, (ROW_COUNT, TOP_K), jnp.float32, 0.2, 0.8)
    w_gate = (jax.random.normal(key_wg, (NUM_EXPERTS, MODEL_DIM, FFN_DIM), jnp.float32) * MODEL_DIM ** -0.5).astype(jnp.bfloat16)
    w_up = (jax.random.normal(key_wu, (NUM_EXPERTS, MODEL_DIM, FFN_DIM), jnp.float32) * MODEL_DIM ** -0.5).astype(jnp.bfloat16)
    w_down = (jax.random.normal(key_wd, (NUM_EXPERTS, FFN_DIM, MODEL_DIM), jnp.float32) * (2.0 * FFN_DIM ** -0.5)).astype(jnp.bfloat16)
    return {'tokens': tokens, 'expert_idx': expert_idx, 'gates': gates, 'w_gate': w_gate, 'w_up': w_up, 'w_down': w_down}


def block_slots(idx_block):
    flat_ids = idx_block.reshape(TOK_DEV * TOP_K)
    onehot = (flat_ids[:, None] == jnp.arange(NUM_EXPERTS)[None, :]).astype(jnp.int32)
    before = jnp.cumsum(onehot, axis=0) - onehot
    return jnp.sum(before * onehot, axis=1)


def reference(tokens, expert_idx, gates, w_gate, w_up, w_down):
    pair_count = ROW_COUNT * TOP_K
    slot_ids = lax.map(block_slots, expert_idx.reshape(GROUP_DEVS, TOK_DEV, TOP_K)).reshape(pair_count)
    flat_ids = expert_idx.reshape(pair_count)
    pair_pos = jnp.arange(pair_count)
    block_id = pair_pos // (TOK_DEV * TOP_K)
    tok_row = (pair_pos // TOP_K).astype(jnp.int32)
    per_expert = GROUP_DEVS * CAPACITY
    total_rows = NUM_EXPERTS * per_expert
    target = jnp.where(slot_ids < CAPACITY, flat_ids * per_expert + block_id * CAPACITY + slot_ids, total_rows)
    row_of = jnp.full((total_rows,), ROW_COUNT, jnp.int32).at[target].set(tok_row, mode='drop')
    gate_of = jnp.zeros((total_rows,), jnp.float32).at[target].set(gates.reshape(pair_count), mode='drop')
    padded = jnp.concatenate([tokens, jnp.zeros((1, MODEL_DIM), tokens.dtype)], axis=0)

    def expert_step(acc, stacked):
        wg_one, wu_one, wd_one, rows_one, gate_one = stacked
        picked = padded[rows_one]
        act_a = jnp.dot(picked, wg_one, preferred_element_type=jnp.float32)
        act_b = jnp.dot(picked, wu_one, preferred_element_type=jnp.float32)
        hidden = (jax.nn.silu(act_a) * act_b).astype(jnp.bfloat16)
        expert_out = jnp.dot(hidden, wd_one, preferred_element_type=jnp.float32).astype(jnp.bfloat16)
        acc = acc.at[rows_one].add(gate_one[:, None] * expert_out.astype(jnp.float32), mode='drop')
        return acc, None

    acc_init = jnp.zeros((ROW_COUNT, MODEL_DIM), jnp.float32)
    acc, unused = lax.scan(expert_step, acc_init, (w_gate, w_up, w_down, row_of.reshape(NUM_EXPERTS, per_expert), gate_of.reshape(NUM_EXPERTS, per_expert)))
    return (tokens.astype(jnp.float32) + acc).astype(jnp.bfloat16)
```

```python
import functools

import jax
import jax.numpy as jnp
from jax import lax
from jax.experimental import pallas as pl
from jax.experimental.pallas import tpu as pltpu
from jax.sharding import PartitionSpec as P

MESH = pl.DeviceIdType.MESH
BF16 = jnp.bfloat16
F32 = jnp.float32

RING = 4
CHUNKS = 10
UNITS = 3
PIECES = 6


def moe_kernel(cap, tok_in, idx_ref, gates_ref, wg, wu, wd, out_ref, gu_land, d_land,
               tok, wbuf, hid, wdb, accs, in_a, in_b, in_l, in_r, gsrc, grecv, gcol,
               tload, tsend, trecv, tfar, gsend, grsem,
               ysend, ssend, from_l, from_r, far_a, far_b, from_s,
               dysend, dssend, dfrom_l, dfrom_r, dfar_a, dfar_b, dfrom_s,
               lsem, dlsem, asend, asem, bsem, lsum, rsum):
    rows = tok_in.shape[0]
    half = rows // 2
    n_local, shard, ffn = wg.shape
    fh = ffn // 2
    hs = shard // 2
    top_k = idx_ref.shape[1]
    unit = shard // UNITS

    q = lax.axis_index('fsdp')
    ep = lax.axis_index('ep')
    chip = ep // 2
    core = ep % 2
    q_l, q_r, q_f = (q + 3) % RING, (q + 1) % RING, (q + 2) % RING
    y_r, y_l = {'fsdp': q_r}, {'fsdp': q_l}
    x_r = {'ep': ((chip + 1) % RING) * 2 + core}
    x_l = {'ep': ((chip + 3) % RING) * 2 + core}
    x_f = {'ep': ((chip + 2) % RING) * 2 + core}
    sib = {'ep': chip * 2 + 1 - core}
    mine = core * n_local
    theirs = (1 - core) * n_local

    def wait(ref, sem):
        pltpu.make_async_copy(ref, ref, sem).wait()

    def send(src, dst, ssem, rsem, dev):
        pltpu.make_async_remote_copy(src_ref=src, dst_ref=dst, send_sem=ssem, recv_sem=rsem,
                                     device_id=dev, device_id_type=MESH).start()

    def fcols(f):
        return pl.ds(pl.multiple_of(f * fh, fh), fh)

    def own_gu(n):
        e, f = n // 2, n % 2
        for dev, ssem, rsem in ((y_r, ysend, from_l), (y_l, ysend, from_r), (sib, ssend, from_s)):
            for m, w in enumerate((wg, wu)):
                send(w.at[e, :, fcols(f)], gu_land.at[mine + e, f, q, m], ssem.at[n], rsem.at[n], dev)

    def fwd_gu(n):
        e, f = n // 2, n % 2
        lref = gu_land.at[mine + e, f, q_l]
        rref = gu_land.at[mine + e, f, q_r]
        wait(lref, from_l.at[n])
        la = gu_land.at[mine + e, f, q_l, :, 0:hs, :]
        send(la, la, ysend.at[n], far_a.at[n], y_r)
        wait(rref, from_r.at[n])
        rb = gu_land.at[mine + e, f, q_r, :, hs:shard, :]
        send(rb, rb, ysend.at[n], far_b.at[n], y_l)
        send(lref, lref, ssend.at[n], from_s.at[n], sib)
        send(rref, rref, ssend.at[n], from_s.at[n], sib)

    def far_gu(n):
        e, f = n // 2, n % 2
        wait(gu_land.at[mine + e, f, q_f, :, 0:hs, :], far_a.at[n])
        wait(gu_land.at[mine + e, f, q_f, :, hs:shard, :], far_b.at[n])
        fref = gu_land.at[mine + e, f, q_f]
        send(fref, fref, ssend.at[n], from_s.at[n], sib)

    def own_d():
        for dev, ssem, rsem in ((y_r, dysend, dfrom_l), (y_l, dysend, dfrom_r)):
            for j in range(UNITS):
                send(wd.at[:, :, j * unit:(j + 1) * unit], d_land.at[q * UNITS + j, pl.ds(mine, n_local)],
                     ssem.at[j], rsem.at[j], dev)

    def own_d_sib():
        for j in range(UNITS):
            send(wd.at[:, :, j * unit:(j + 1) * unit], d_land.at[q * UNITS + j, pl.ds(mine, n_local)],
                 dssend.at[j], dfrom_s.at[0, j], sib)

    def fwd_d(j):
        lref = d_land.at[q_l * UNITS + j, pl.ds(mine, n_local)]
        rref = d_land.at[q_r * UNITS + j, pl.ds(mine, n_local)]
        wait(lref, dfrom_l.at[j])
        la = d_land.at[q_l * UNITS + j, pl.ds(mine, n_local), 0:fh]
        send(la, la, dysend.at[j], dfar_a.at[j], y_r)
        wait(rref, dfrom_r.at[j])
        rb = d_land.at[q_r * UNITS + j, pl.ds(mine, n_local), fh:ffn]
        send(rb, rb, dysend.at[j], dfar_b.at[j], y_l)
        send(lref, lref, dssend.at[j], dfrom_s.at[1, j], sib)
        send(rref, rref, dssend.at[j], dfrom_s.at[2, j], sib)

    def far_d(j):
        wait(d_land.at[q_f * UNITS + j, pl.ds(mine, n_local), 0:fh], dfar_a.at[j])
        wait(d_land.at[q_f * UNITS + j, pl.ds(mine, n_local), fh:ffn], dfar_b.at[j])
        fref = d_land.at[q_f * UNITS + j, pl.ds(mine, n_local)]
        send(fref, fref, dssend.at[j], dfrom_s.at[3, j], sib)

    def load_mine(n):
        e, f = n // 2, n % 2
        for m, w in enumerate((wg, wu)):
            pltpu.make_async_copy(w.at[e, :, fcols(f)], wbuf.at[0, q, :, m * fh:(m + 1) * fh], lsem.at[0]).start()
            for other in (q_l, q_r, q_f):
                pltpu.make_async_copy(gu_land.at[mine + e, f, other, m],
                                      wbuf.at[0, other, :, m * fh:(m + 1) * fh], lsem.at[0]).start()

    def load_theirs(n):
        e, f = n // 2, n % 2
        wait(gu_land.at[theirs + e, f], from_s.at[n])
        for m in range(2):
            pltpu.make_async_copy(gu_land.at[theirs + e, f, :, m],
                                  wbuf.at[1, :, :, m * fh:(m + 1) * fh], lsem.at[1]).start()

    def seq_unit(s):
        if s < 3:
            return 0, s
        if s < 9:
            return (1 if s % 2 else 2), (s - 3) // 2
        return 3, s - 9

    shards = (q, q_l, q_r, q_f)

    def load_piece(p):
        for i in range(2):
            kind, j = seq_unit(2 * p + i)
            gid = shards[kind] * UNITS + j
            lanes = slice(i * unit, (i + 1) * unit)
            wait(d_land.at[gid, pl.ds(theirs, n_local)], dfrom_s.at[kind, j])
            if kind == 0:
                pltpu.make_async_copy(wd.at[:, :, j * unit:(j + 1) * unit],
                                      wdb.at[p % 2, pl.ds(mine, n_local), :, lanes], dlsem.at[p % 2]).start()
                pltpu.make_async_copy(d_land.at[gid, pl.ds(theirs, n_local)],
                                      wdb.at[p % 2, pl.ds(theirs, n_local), :, lanes], dlsem.at[p % 2]).start()
            else:
                pltpu.make_async_copy(d_land.at[gid], wdb.at[p % 2, :, :, lanes], dlsem.at[p % 2]).start()

    barrier = pltpu.get_barrier_semaphore()
    for dev in (y_r, y_l, x_r, x_l, x_f, sib):
        pl.semaphore_signal(barrier, inc=1, device_id=dev, device_id_type=MESH)
    pl.semaphore_wait(barrier, 6)

    own_tok = pltpu.make_async_copy(tok_in, tok.at[0], tload)
    own_tok.start()
    send(tok_in, tok.at[1], tsend.at[0], trecv.at[0], x_r)
    send(tok_in, tok.at[2], tsend.at[1], trecv.at[1], x_l)
    own_gu(0)
    own_gu(1)
    own_d_sib()

    lane = lax.broadcasted_iota(jnp.int32, (rows, 128), 1)
    chosen = jnp.zeros((rows, 128), F32)
    gval = jnp.zeros((rows, 128), F32)
    for j in range(top_k):
        hit = idx_ref[:, j:j + 1] == lane
        chosen = jnp.where(hit, 1.0, chosen)
        gval = jnp.where(hit, gates_ref[:, j:j + 1], gval)
    earlier = lax.broadcasted_iota(jnp.int32, (rows, rows), 1) < lax.broadcasted_iota(jnp.int32, (rows, rows), 0)
    before = jnp.dot(jnp.where(earlier, 1.0, 0.0).astype(BF16), chosen.astype(BF16), preferred_element_type=F32)
    gsrc[...] = jnp.where(before < cap - 0.5, gval, 0.0)

    fwd_gu(0)
    own_gu(2)
    fwd_gu(1)
    own_gu(3)
    far_gu(0)
    fwd_gu(2)
    own_gu(4)
    wait(tok.at[1], trecv.at[0])
    ta = tok.at[1, 0:half]
    send(ta, tok.at[3, 0:half], tsend.at[2], tfar.at[0], x_r)
    wait(tok.at[2], trecv.at[1])
    tb = tok.at[2, half:rows]
    send(tb, tok.at[3, half:rows], tsend.at[3], tfar.at[1], x_l)
    for i, dev in enumerate((x_r, x_l, x_f)):
        send(gsrc, grecv.at[i], gsend.at[i], grsem.at[i], dev)
    far_gu(1)
    fwd_gu(3)
    own_gu(5)
    far_gu(2)
    own_tok.wait()
    load_mine(0)
    wait(tok.at[3, 0:half], tfar.at[0])
    wait(tok.at[3, half:rows], tfar.at[1])

    def gu_unit(u, slot, n):
        e, f = n // 2, n % 2
        base = jnp.where(slot == 0, mine, theirs)

        def block(b, carry):
            both = jnp.dot(tok[b], wbuf[slot].reshape(RING * shard, ffn), preferred_element_type=F32)
            act_a, act_b = both[:, :fh], both[:, fh:]
            hid[base + e, b, :, fcols(f)] = (act_a * jax.nn.sigmoid(act_a) * act_b).astype(BF16)
            return carry
        return block

    def unit_step(u, carry):
        n, slot = u // 2, u % 2
        wait(wbuf.at[slot], lsem.at[slot])
        block = gu_unit(u, slot, n)
        lax.fori_loop(0, 2, block, 0)

        @pl.when((u % 3 == 1) & (u <= 16))
        def _():
            fwd_gu(4 + u // 3)

            @pl.when(u <= 10)
            def _():
                own_gu(6 + u // 3)

            @pl.when(u == 16)
            def _():
                own_d()

        for k, step in ((3, 2), (4, 5), (5, 8), (6, 11), (7, 13), (8, 15), (9, 17)):
            @pl.when(u == step)
            def _(k=k):
                far_gu(k)

        @pl.when(slot == 0)
        def _():
            load_theirs(n)

        @pl.when((slot == 1) & (n < CHUNKS - 1))
        def _():
            load_mine(n + 1)

        @pl.when(u == 18)
        def _():
            load_piece(0)

        lax.fori_loop(2, 4, block, 0)
        return carry

    lax.fori_loop(0, 2 * CHUNKS, unit_step, 0)

    shift = (128 - chip * 2 * n_local) % 128
    gcol[0] = pltpu.roll(gsrc[...], shift, 1)
    for i in range(3):
        wait(grecv.at[i], grsem.at[i])
        gcol[i + 1] = pltpu.roll(grecv[i], shift, 1)

    def finish(p):
        s = p % 2
        wait(in_l.at[p], lsum.at[p])
        wait(in_r.at[p], rsum.at[p])
        for i in range(2):
            if isinstance(p, int):
                kind, j = seq_unit(2 * p + i)
                gid = shards[kind] * UNITS + j
            else:
                sq = 2 * p + i
                mid = sq - 3
                kind = jnp.where(sq < 3, 0, jnp.where(sq < 9, 1 + mid % 2, 3))
                j = jnp.where(sq < 3, sq, jnp.where(sq < 9, mid // 2, sq - 9))
                sh = jnp.where(kind == 0, q, jnp.where(kind == 1, q_l, jnp.where(kind == 2, q_r, q_f)))
                gid = sh * UNITS + j
            cols = pl.ds(pl.multiple_of(gid * unit, unit), unit)
            lanes = slice(i * unit, (i + 1) * unit)
            total = accs[s, 3, :, lanes] + in_l[p, :, lanes] + in_r[p, :, lanes]
            out_ref[:, cols] = (tok[0, :, cols].astype(F32) + total).astype(BF16)

    def block_step(t, carry):
        p, i = t // 4, t % 4
        s = p % 2
        b = 3 - i

        @pl.when(i == 0)
        def _():
            wait(wdb.at[s], dlsem.at[s])

        @pl.when((p >= 2) & (i < 3))
        def _():
            wait(accs.at[s, i], asend.at[p - 2, i])

        gates_b = gcol[b]
        total = None
        for e in range(2 * n_local):
            o = jnp.dot(hid[e, b], wdb[s, e], preferred_element_type=F32).astype(BF16).astype(F32)
            g = gates_b[:, e:e + 1]
            o = jnp.where(g != 0.0, g * o, 0.0)
            total = o if total is None else total + o
        accs[s, i] = total

        @pl.when(i == 0)
        def _():
            send(accs.at[s, 0, 0:half], in_a.at[p], asend.at[p, 0], asem.at[p], x_r)
            send(accs.at[s, 0, half:rows], in_b.at[p], asend.at[p, 0], bsem.at[p], x_l)

            @pl.when(p == 1)
            def _():
                fwd_d(1)

            @pl.when(p == 2)
            def _():
                fwd_d(2)

            @pl.when(p == 3)
            def _():
                far_d(0)

            @pl.when(p == 4)
            def _():
                far_d(1)
                far_d(2)

        @pl.when(i == 1)
        def _():
            send(accs.at[s, 1, half:rows], in_l.at[p, half:rows], asend.at[p, 1], lsum.at[p], x_r)

        @pl.when(i == 2)
        def _():
            send(accs.at[s, 2, 0:half], in_r.at[p, 0:half], asend.at[p, 2], rsum.at[p], x_l)
            wait(in_a.at[p], asem.at[p])
            accs[s, 1, 0:half] += in_a[p]
            send(accs.at[s, 1, 0:half], in_l.at[p, 0:half], asend.at[p, 1], lsum.at[p], x_r)
            wait(in_b.at[p], bsem.at[p])
            accs[s, 2, half:rows] += in_b[p]
            send(accs.at[s, 2, half:rows], in_r.at[p, half:rows], asend.at[p, 2], rsum.at[p], x_l)

            @pl.when(p == 0)
            def _():
                fwd_d(0)

            for k in range(1, PIECES):
                @pl.when(p == k - 1)
                def _(k=k):
                    load_piece(k)

        @pl.when((i == 3) & (p >= 1))
        def _():
            finish(p - 1)
        return carry

    lax.fori_loop(0, 4 * PIECES, block_step, 0)
    finish(PIECES - 1)

    def drain(n, carry):
        wait(gu_land.at[0, 0, 0:3], ysend.at[n])
        wait(gu_land.at[0, 0], ssend.at[n])
        return carry

    lax.fori_loop(0, CHUNKS, drain, 0)
    for j in range(UNITS):
        wait(d_land.at[0:3, 0:n_local], dysend.at[j])
        wait(d_land.at[0:4, 0:n_local], dssend.at[j])
    wait(tok.at[1], tsend.at[0])
    wait(tok.at[1], tsend.at[1])
    wait(tok.at[1, 0:half], tsend.at[2])
    wait(tok.at[1, 0:half], tsend.at[3])
    for i in range(3):
        wait(gsrc, gsend.at[i])
    for p in (PIECES - 2, PIECES - 1):
        for i in range(3):
            wait(accs.at[0, 0], asend.at[p, i])


def solution(mesh):
    ep_size = mesh.shape['ep']
    row_spec = P(('rep', 'ep', 'fsdp'), None)

    def device_step(tokens, expert_idx, gates, w_gate, w_up, w_down):
        rows, top_k = expert_idx.shape
        n_local, shard, ffn = w_gate.shape
        model_dim = tokens.shape[1]
        num_experts = n_local * ep_size
        cap = (2 * rows * top_k + num_experts - 1) // num_experts
        fh, half, unit = ffn // 2, rows // 2, shard // UNITS
        piece = 2 * unit
        vmem = pl.BlockSpec(memory_space=pltpu.VMEM)
        hbm = pl.BlockSpec(memory_space=pl.ANY)
        dma = pltpu.SemaphoreType.DMA
        out, _, _ = pl.pallas_call(
            functools.partial(moe_kernel, cap),
            out_shape=(
                jax.ShapeDtypeStruct((rows, model_dim), BF16),
                jax.ShapeDtypeStruct((2 * n_local, 2, RING, 2, shard, fh), BF16),
                jax.ShapeDtypeStruct((RING * UNITS, 2 * n_local, ffn, unit), BF16),
            ),
            in_specs=[hbm, vmem, vmem, hbm, hbm, hbm],
            out_specs=(vmem, hbm, hbm),
            scratch_shapes=[
                pltpu.VMEM((4, rows, model_dim), BF16),
                pltpu.VMEM((2, RING, shard, ffn), BF16),
                pltpu.VMEM((2 * n_local, 4, rows, ffn), BF16),
                pltpu.VMEM((2, 2 * n_local, ffn, piece), BF16),
                pltpu.VMEM((2, 4, rows, piece), F32),
                pltpu.VMEM((PIECES, half, piece), F32),
                pltpu.VMEM((PIECES, half, piece), F32),
                pltpu.VMEM((PIECES, rows, piece), F32),
                pltpu.VMEM((PIECES, rows, piece), F32),
                pltpu.VMEM((rows, 128), F32),
                pltpu.VMEM((3, rows, 128), F32),
                pltpu.VMEM((4, rows, 128), F32),
                dma, dma((4,)), dma((2,)), dma((2,)), dma((3,)), dma((3,)),
                dma((CHUNKS,)), dma((CHUNKS,)), dma((CHUNKS,)), dma((CHUNKS,)), dma((CHUNKS,)), dma((CHUNKS,)), dma((CHUNKS,)),
                dma((UNITS,)), dma((UNITS,)), dma((UNITS,)), dma((UNITS,)), dma((UNITS,)), dma((UNITS,)), dma((4, UNITS)),
                dma((2,)), dma((2,)), dma((PIECES, 3)), dma((PIECES,)), dma((PIECES,)), dma((PIECES,)), dma((PIECES,)),
            ],
            compiler_params=pltpu.CompilerParams(collective_id=0, has_side_effects=True, vmem_limit_bytes=67043328),
            name='moe_ring',
        )(tokens, expert_idx, gates, w_gate, w_up, w_down)
        return out

    return jax.shard_map(device_step, mesh=mesh, in_specs=(row_spec, row_spec, row_spec, P('ep', 'fsdp', None), P('ep', 'fsdp', None), P('ep', None, 'fsdp')), out_specs=row_spec, check_vma=False)
```

```python
import functools

import jax
import jax.numpy as jnp
from jax import lax
from jax.experimental import pallas as pl
from jax.experimental.pallas import tpu as pltpu
from jax.sharding import PartitionSpec as P

MESH = pl.DeviceIdType.MESH
BF16 = jnp.bfloat16
F32 = jnp.float32

RING = 4
CHUNKS = 10
UNITS = 3
PIECES = 6


def moe_kernel(cap, tok_in, idx_ref, gates_ref, wg, wu, wd, out_ref, gu_land, d_land,
               tok, wbuf, hid, wdb, wlast, accs, in_a, in_b, in_l, in_r, gsrc, grecv, gcol, stage,
               tload, tsend, trecv, tfar, gsend, grsem,
               ysend, ssend, from_l, from_r, far_a, far_b, from_s,
               dysend, dssend, dfrom_l, dfrom_r, dfar_a, dfar_b, dfrom_s,
               lsem, dlsem, asend, asem, bsem, lsum, rsum, osem, efwd):
    rows = tok_in.shape[0]
    half = rows // 2
    n_local, shard, ffn = wg.shape
    fh = ffn // 2
    hs = shard // 2
    top_k = idx_ref.shape[0]
    unit = shard // UNITS

    q = lax.axis_index('fsdp')
    ep = lax.axis_index('ep')
    chip = ep // 2
    core = ep % 2
    q_l, q_r, q_f = (q + 3) % RING, (q + 1) % RING, (q + 2) % RING
    y_r, y_l = {'fsdp': q_r}, {'fsdp': q_l}
    x_r = {'ep': ((chip + 1) % RING) * 2 + core}
    x_l = {'ep': ((chip + 3) % RING) * 2 + core}
    x_f = {'ep': ((chip + 2) % RING) * 2 + core}
    sib = {'ep': chip * 2 + 1 - core}
    mine = core * n_local
    theirs = (1 - core) * n_local

    def wait(ref, sem):
        pltpu.make_async_copy(ref, ref, sem).wait()

    def send(src, dst, ssem, rsem, dev):
        pltpu.make_async_remote_copy(src_ref=src, dst_ref=dst, send_sem=ssem, recv_sem=rsem,
                                     device_id=dev, device_id_type=MESH).start()

    def fcols(f):
        return pl.ds(pl.multiple_of(f * fh, fh), fh)

    def own_gu(n):
        e, f = n // 2, n % 2
        for dev, ssem, rsem in ((y_r, ysend, from_l), (y_l, ysend, from_r), (sib, ssend, from_s)):
            for m, w in enumerate((wg, wu)):
                send(w.at[e, :, fcols(f)], gu_land.at[mine + e, f, q, m], ssem.at[n], rsem.at[n], dev)

    def fwd_gu(n):
        e, f = n // 2, n % 2
        lref = gu_land.at[mine + e, f, q_l]
        rref = gu_land.at[mine + e, f, q_r]
        wait(lref, from_l.at[n])
        la = gu_land.at[mine + e, f, q_l, :, 0:hs, :]
        send(la, la, ysend.at[n], far_a.at[n], y_r)
        wait(rref, from_r.at[n])
        rb = gu_land.at[mine + e, f, q_r, :, hs:shard, :]
        send(rb, rb, ysend.at[n], far_b.at[n], y_l)
        send(lref, lref, ssend.at[n], from_s.at[n], sib)
        send(rref, rref, ssend.at[n], from_s.at[n], sib)

    def far_gu(n):
        e, f = n // 2, n % 2
        wait(gu_land.at[mine + e, f, q_f, :, 0:hs, :], far_a.at[n])
        wait(gu_land.at[mine + e, f, q_f, :, hs:shard, :], far_b.at[n])
        fref = gu_land.at[mine + e, f, q_f]
        send(fref, fref, ssend.at[n], from_s.at[n], sib)

    last = CHUNKS - 1
    le, lf = last // 2, last % 2
    top, low = slice(0, hs), slice(hs, shard)

    def to_sib_last(shard_id, ref):
        for m in range(2):
            send(ref(m), wlast.at[shard_id, :, m * fh:(m + 1) * fh], ssend.at[last], from_s.at[last], sib)

    def own_last():
        for dev, order, early, late in ((y_r, (top, low), 0, from_l), (y_l, (low, top), 1, from_r)):
            for part, rsem in zip(order, (efwd.at[early], late.at[last])):
                for m, w in enumerate((wg, wu)):
                    send(w.at[le, part, lf * fh:(lf + 1) * fh], gu_land.at[mine + le, lf, q, m, part],
                         ysend.at[last], rsem, dev)
        to_sib_last(q, lambda m: (wg, wu)[m].at[le, :, lf * fh:(lf + 1) * fh])

    def fwd_last():
        la = gu_land.at[mine + le, lf, q_l, :, top]
        wait(la, efwd.at[0])
        send(la, la, ysend.at[last], far_a.at[last], y_r)
        rb = gu_land.at[mine + le, lf, q_r, :, low]
        wait(rb, efwd.at[1])
        send(rb, rb, ysend.at[last], far_b.at[last], y_l)

    def near_last():
        wait(gu_land.at[mine + le, lf, q_l, :, low], from_l.at[last])
        to_sib_last(q_l, lambda m: gu_land.at[mine + le, lf, q_l, m])
        wait(gu_land.at[mine + le, lf, q_r, :, top], from_r.at[last])
        to_sib_last(q_r, lambda m: gu_land.at[mine + le, lf, q_r, m])

    def far_last():
        wait(gu_land.at[mine + le, lf, q_f, :, top], far_a.at[last])
        wait(gu_land.at[mine + le, lf, q_f, :, low], far_b.at[last])
        to_sib_last(q_f, lambda m: gu_land.at[mine + le, lf, q_f, m])

    def own_d():
        for dev, ssem, rsem in ((y_r, dysend, dfrom_l), (y_l, dysend, dfrom_r)):
            for j in range(UNITS):
                send(wd.at[:, :, j * unit:(j + 1) * unit], d_land.at[q * UNITS + j, pl.ds(mine, n_local)],
                     ssem.at[j], rsem.at[j], dev)

    def own_d_sib():
        for j in range(UNITS):
            send(wd.at[:, :, j * unit:(j + 1) * unit], d_land.at[q * UNITS + j, pl.ds(mine, n_local)],
                 dssend.at[j], dfrom_s.at[0, j], sib)

    def fwd_d(j):
        lref = d_land.at[q_l * UNITS + j, pl.ds(mine, n_local)]
        rref = d_land.at[q_r * UNITS + j, pl.ds(mine, n_local)]
        wait(lref, dfrom_l.at[j])
        la = d_land.at[q_l * UNITS + j, pl.ds(mine, n_local), 0:fh]
        send(la, la, dysend.at[j], dfar_a.at[j], y_r)
        wait(rref, dfrom_r.at[j])
        rb = d_land.at[q_r * UNITS + j, pl.ds(mine, n_local), fh:ffn]
        send(rb, rb, dysend.at[j], dfar_b.at[j], y_l)
        send(lref, lref, dssend.at[j], dfrom_s.at[1, j], sib)
        send(rref, rref, dssend.at[j], dfrom_s.at[2, j], sib)

    def far_d(j):
        wait(d_land.at[q_f * UNITS + j, pl.ds(mine, n_local), 0:fh], dfar_a.at[j])
        wait(d_land.at[q_f * UNITS + j, pl.ds(mine, n_local), fh:ffn], dfar_b.at[j])
        fref = d_land.at[q_f * UNITS + j, pl.ds(mine, n_local)]
        send(fref, fref, dssend.at[j], dfrom_s.at[3, j], sib)

    def load_mine(n):
        e, f, par = n // 2, n % 2, n % 2
        for m, w in enumerate((wg, wu)):
            lanes = slice(m * fh, (m + 1) * fh)
            pltpu.make_async_copy(w.at[e, :, fcols(f)], wbuf.at[par, 0, q, :, lanes], lsem.at[par, 0]).start()
            for other in (q_l, q_r, q_f):
                pltpu.make_async_copy(gu_land.at[mine + e, f, other, m],
                                      wbuf.at[par, 0, other, :, lanes], lsem.at[par, 0]).start()

    def load_theirs(n, again=False):
        e, f, par = n // 2, n % 2, n % 2
        if not again:
            wait(gu_land.at[theirs + e, f], from_s.at[n])
        for m in range(2):
            pltpu.make_async_copy(gu_land.at[theirs + e, f, :, m],
                                  wbuf.at[par, 1, :, :, m * fh:(m + 1) * fh], lsem.at[par, 1]).start()

    def loaded(n, side):
        wait(wbuf.at[n % 2, side], lsem.at[n % 2, side])

    def seq_unit(s):
        if s < 3:
            return 0, s
        if s < 9:
            return (1 if s % 2 else 2), (s - 3) // 2
        return 3, s - 9

    shards = (q, q_l, q_r, q_f)

    def load_piece(p):
        for i in range(2):
            kind, j = seq_unit(2 * p + i)
            gid = shards[kind] * UNITS + j
            lanes = slice(i * unit, (i + 1) * unit)
            wait(d_land.at[gid, pl.ds(theirs, n_local)], dfrom_s.at[kind, j])
            if kind == 0:
                pltpu.make_async_copy(wd.at[:, :, j * unit:(j + 1) * unit],
                                      wdb.at[p % 2, pl.ds(mine, n_local), :, lanes], dlsem.at[p % 2]).start()
                pltpu.make_async_copy(d_land.at[gid, pl.ds(theirs, n_local)],
                                      wdb.at[p % 2, pl.ds(theirs, n_local), :, lanes], dlsem.at[p % 2]).start()
            else:
                pltpu.make_async_copy(d_land.at[gid], wdb.at[p % 2, :, :, lanes], dlsem.at[p % 2]).start()

    barrier = pltpu.get_barrier_semaphore()
    for dev in (y_r, y_l, x_r, x_l, x_f, sib):
        pl.semaphore_signal(barrier, inc=1, device_id=dev, device_id_type=MESH)
    pl.semaphore_wait(barrier, 6)

    own_tok = pltpu.make_async_copy(tok_in, tok.at[0], tload)
    own_tok.start()
    send(tok_in, tok.at[1], tsend.at[0], trecv.at[0], x_r)
    send(tok_in, tok.at[2], tsend.at[1], trecv.at[1], x_l)
    own_gu(0)
    own_gu(1)
    own_d_sib()

    expert = lax.broadcasted_iota(jnp.int32, (128, rows), 0)
    chosen = jnp.zeros((128, rows), F32)
    gval = jnp.zeros((128, rows), F32)
    for j in range(top_k):
        hit = idx_ref[j:j + 1, :] == expert
        chosen = jnp.where(hit, 1.0, chosen)
        gval = jnp.where(hit, gates_ref[j:j + 1, :], gval)
    earlier = lax.broadcasted_iota(jnp.int32, (rows, rows), 0) < lax.broadcasted_iota(jnp.int32, (rows, rows), 1)
    before = jnp.dot(chosen.astype(BF16), jnp.where(earlier, 1.0, 0.0).astype(BF16), preferred_element_type=F32)
    gsrc[...] = jnp.where(before < cap - 0.5, gval, 0.0).T

    fwd_gu(0)
    own_gu(2)
    fwd_gu(1)
    own_gu(3)
    far_gu(0)
    load_mine(0)
    load_theirs(0)
    fwd_gu(2)
    own_gu(4)
    wait(tok.at[1], trecv.at[0])
    ta = tok.at[1, 0:half]
    send(ta, tok.at[3, 0:half], tsend.at[2], tfar.at[0], x_r)
    wait(tok.at[2], trecv.at[1])
    tb = tok.at[2, half:rows]
    send(tb, tok.at[3, half:rows], tsend.at[3], tfar.at[1], x_l)
    for i, dev in enumerate((x_r, x_l, x_f)):
        send(gsrc, grecv.at[i], gsend.at[i], grsem.at[i], dev)
    far_gu(1)
    load_mine(1)
    load_theirs(1)
    own_tok.wait()

    def gu_item(n, side, b, weights=None):
        e, f, par = n // 2, n % 2, n % 2
        w = wbuf[par, side] if weights is None else weights[...]
        both = jnp.dot(tok[b], w.reshape(RING * shard, ffn), preferred_element_type=F32)
        act_a, act_b = both[:, :fh], both[:, fh:]
        base = jnp.where(side == 0, mine, theirs)
        hid[base + e, b, :, fcols(f)] = (act_a * jax.nn.sigmoid(act_a) * act_b).astype(BF16)

    def gu_items(n, side, b0, b1):
        def body(b, carry):
            gu_item(n, side, b)
            return carry
        lax.fori_loop(b0, b1, body, 0)

    def early(n, carry):
        def side_step(side, c):
            loaded(n, side)
            gu_items(n, side, 0, 3)

            @pl.when((n == 0) & (side == 1))
            def _():
                fwd_gu(3)
                own_gu(5)

            @pl.when((n == 1) & (side == 0))
            def _():
                far_gu(2)
                load_mine(2)

            @pl.when((n == 1) & (side == 1))
            def _():
                load_theirs(2)
            return c
        lax.fori_loop(0, 2, side_step, 0)
        return carry

    lax.fori_loop(0, 3, early, 0)
    wait(tok.at[3, 0:half], tfar.at[0])
    wait(tok.at[3, half:rows], tfar.at[1])

    def late(k, carry):
        n, side = 2 - k // 2, k % 2

        @pl.when(n == 0)
        def _():
            loaded(n, side)
        gu_item(n, side, 3)

        @pl.when(k == 1)
        def _():
            load_mine(0)
            load_theirs(0, again=True)
            fwd_gu(4)
            own_gu(6)

        @pl.when(k == 4)
        def _():
            far_gu(3)
            load_mine(3)
        return carry

    lax.fori_loop(0, 6, late, 0)
    load_theirs(3)

    def steady(n, carry):
        loaded(n, 0)
        gu_items(n, 0, 0, 4)

        @pl.when(n == CHUNKS - 2)
        def _():
            near_last()
            own_d()
            load_piece(0)

        loaded(n, 1)
        gu_items(n, 1, 0, 2)

        @pl.when(n <= CHUNKS - 4)
        def _():
            fwd_gu(n + 2)

            @pl.when(n <= 4)
            def _():
                own_gu(n + 4)

            @pl.when(n == CHUNKS - 4)
            def _():
                own_last()

        @pl.when(n <= CHUNKS - 3)
        def _():
            far_gu(n + 1)
            load_mine(n + 1)

        gu_items(n, 1, 2, 4)

        @pl.when(n <= CHUNKS - 3)
        def _():
            load_theirs(n + 1)

        @pl.when(n == CHUNKS - 3)
        def _():
            fwd_last()

        @pl.when(n == 5)
        def _():
            shift = (128 - chip * 2 * n_local) % 128
            gcol[0] = pltpu.roll(gsrc[...], shift, 1)
            for i in range(3):
                wait(grecv.at[i], grsem.at[i])
                gcol[i + 1] = pltpu.roll(grecv[i], shift, 1)
        return carry

    lax.fori_loop(3, CHUNKS - 1, steady, 0)
    far_last()
    load_mine(last)

    def finish(p):
        s = p % 2
        wait(in_l.at[p], lsum.at[p])
        wait(in_r.at[p], rsum.at[p])
        for i in range(2):
            if isinstance(p, int):
                kind, j = seq_unit(2 * p + i)
                gid = shards[kind] * UNITS + j
            else:
                sq = 2 * p + i
                mid = sq - 3
                kind = jnp.where(sq < 3, 0, jnp.where(sq < 9, 1 + mid % 2, 3))
                j = jnp.where(sq < 3, sq, jnp.where(sq < 9, mid // 2, sq - 9))
                sh = jnp.where(kind == 0, q, jnp.where(kind == 1, q_l, jnp.where(kind == 2, q_r, q_f)))
                gid = sh * UNITS + j
            cols = pl.ds(pl.multiple_of(gid * unit, unit), unit)
            lanes = slice(i * unit, (i + 1) * unit)
            total = accs[s, 3, :, lanes] + in_l[p, :, lanes] + in_r[p, :, lanes]
            stage[:, cols] = (tok[0, :, cols].astype(F32) + total).astype(BF16)
            pltpu.make_async_copy(stage.at[:, cols], out_ref.at[:, cols], osem.at[p]).start()

    last_experts = (le, n_local + le)
    early_experts = [e for e in range(2 * n_local) if e not in last_experts]

    def combine(s, b, experts):
        gates_b = gcol[b]
        total = None
        for e in experts:
            o = jnp.dot(hid[e, b], wdb[s, e], preferred_element_type=F32).astype(BF16).astype(F32)
            g = gates_b[:, e:e + 1]
            o = jnp.where(g != 0.0, g * o, 0.0)
            total = o if total is None else total + o
        return total

    wait(wdb.at[0], dlsem.at[0])
    accs[0, 0] = combine(0, 3, early_experts)

    def block_step(t, carry):
        p, i = t // 4, t % 4
        s = p % 2
        b = 3 - i

        @pl.when((i == 0) & (p > 0))
        def _():
            wait(wdb.at[s], dlsem.at[s])

        @pl.when((p >= 2) & (i < 3))
        def _():
            wait(accs.at[s, i], asend.at[p - 2, i])

        @pl.when(p == 0)
        def _():
            @pl.when(i > 0)
            def _():
                accs[0, i] = combine(0, b, early_experts)

            @pl.when(i == 0)
            def _():
                loaded(last, 0)
            gu_item(last, 0, b)

            @pl.when(i == 0)
            def _():
                wait(wlast, from_s.at[last])
            gu_item(last, 1, b, wlast)
            accs[0, i] += combine(0, b, last_experts)

        @pl.when(p > 0)
        def _():
            accs[s, i] = combine(s, b, range(2 * n_local))

        @pl.when(i == 0)
        def _():
            send(accs.at[s, 0, 0:half], in_a.at[p], asend.at[p, 0], asem.at[p], x_r)
            send(accs.at[s, 0, half:rows], in_b.at[p], asend.at[p, 0], bsem.at[p], x_l)

            @pl.when(p == 1)
            def _():
                fwd_d(1)

            @pl.when(p == 2)
            def _():
                fwd_d(2)

            @pl.when(p == 3)
            def _():
                far_d(0)

            @pl.when(p == 4)
            def _():
                far_d(1)
                far_d(2)

        @pl.when(i == 1)
        def _():
            send(accs.at[s, 1, half:rows], in_l.at[p, half:rows], asend.at[p, 1], lsum.at[p], x_r)

        @pl.when(i == 2)
        def _():
            send(accs.at[s, 2, 0:half], in_r.at[p, 0:half], asend.at[p, 2], rsum.at[p], x_l)
            wait(in_a.at[p], asem.at[p])
            accs[s, 1, 0:half] += in_a[p]
            send(accs.at[s, 1, 0:half], in_l.at[p, 0:half], asend.at[p, 1], lsum.at[p], x_r)
            wait(in_b.at[p], bsem.at[p])
            accs[s, 2, half:rows] += in_b[p]
            send(accs.at[s, 2, half:rows], in_r.at[p, half:rows], asend.at[p, 2], rsum.at[p], x_l)

            @pl.when(p == 0)
            def _():
                fwd_d(0)

            for k in range(1, PIECES):
                @pl.when(p == k - 1)
                def _(k=k):
                    load_piece(k)

        @pl.when((i == 3) & (p >= 1))
        def _():
            finish(p - 1)
        return carry

    lax.fori_loop(0, 4 * PIECES, block_step, 0)
    finish(PIECES - 1)

    def drain(n, carry):
        wait(gu_land.at[0, 0, 0:3], ysend.at[n])
        wait(gu_land.at[0, 0], ssend.at[n])
        return carry

    lax.fori_loop(0, CHUNKS, drain, 0)
    for j in range(UNITS):
        wait(d_land.at[0:3, 0:n_local], dysend.at[j])
        wait(d_land.at[0:4, 0:n_local], dssend.at[j])
    wait(tok.at[1], tsend.at[0])
    wait(tok.at[1], tsend.at[1])
    wait(tok.at[1, 0:half], tsend.at[2])
    wait(tok.at[1, 0:half], tsend.at[3])
    for i in range(3):
        wait(gsrc, gsend.at[i])
    for p in (PIECES - 2, PIECES - 1):
        for i in range(3):
            wait(accs.at[0, 0], asend.at[p, i])
    for p in range(PIECES):
        wait(stage.at[:, 0:2 * unit], osem.at[p])


def solution(mesh):
    ep_size = mesh.shape['ep']
    row_spec = P(('rep', 'ep', 'fsdp'), None)

    def device_step(tokens, expert_idx, gates, w_gate, w_up, w_down):
        rows, top_k = expert_idx.shape
        n_local, shard, ffn = w_gate.shape
        model_dim = tokens.shape[1]
        num_experts = n_local * ep_size
        cap = (2 * rows * top_k + num_experts - 1) // num_experts
        fh, half, unit = ffn // 2, rows // 2, shard // UNITS
        piece = 2 * unit
        vmem = pl.BlockSpec(memory_space=pltpu.VMEM)
        hbm = pl.BlockSpec(memory_space=pl.ANY)
        dma = pltpu.SemaphoreType.DMA
        out, _, _ = pl.pallas_call(
            functools.partial(moe_kernel, cap),
            out_shape=(
                jax.ShapeDtypeStruct((rows, model_dim), BF16),
                jax.ShapeDtypeStruct((2 * n_local, 2, RING, 2, shard, fh), BF16),
                jax.ShapeDtypeStruct((RING * UNITS, 2 * n_local, ffn, unit), BF16),
            ),
            in_specs=[hbm, vmem, vmem, hbm, hbm, hbm],
            out_specs=(hbm, hbm, hbm),
            scratch_shapes=[
                pltpu.VMEM((4, rows, model_dim), BF16),
                pltpu.VMEM((2, 2, RING, shard, ffn), BF16),
                pltpu.VMEM((2 * n_local, 4, rows, ffn), BF16),
                pltpu.VMEM((2, 2 * n_local, ffn, piece), BF16),
                pltpu.VMEM((RING, shard, ffn), BF16),
                pltpu.VMEM((2, 4, rows, piece), F32),
                pltpu.VMEM((PIECES, half, piece), F32),
                pltpu.VMEM((PIECES, half, piece), F32),
                pltpu.VMEM((PIECES, rows, piece), F32),
                pltpu.VMEM((PIECES, rows, piece), F32),
                pltpu.VMEM((rows, 128), F32),
                pltpu.VMEM((3, rows, 128), F32),
                pltpu.VMEM((4, rows, 128), F32),
                pltpu.VMEM((rows, model_dim), BF16),
                dma, dma((4,)), dma((2,)), dma((2,)), dma((3,)), dma((3,)),
                dma((CHUNKS,)), dma((CHUNKS,)), dma((CHUNKS,)), dma((CHUNKS,)), dma((CHUNKS,)), dma((CHUNKS,)), dma((CHUNKS,)),
                dma((UNITS,)), dma((UNITS,)), dma((UNITS,)), dma((UNITS,)), dma((UNITS,)), dma((UNITS,)), dma((4, UNITS)),
                dma((2, 2)), dma((2,)), dma((PIECES, 3)), dma((PIECES,)), dma((PIECES,)), dma((PIECES,)), dma((PIECES,)), dma((PIECES,)), dma((2,)),
            ],
            compiler_params=pltpu.CompilerParams(collective_id=0, has_side_effects=True, vmem_limit_bytes=67043328),
            name='moe_ring',
        )(tokens, expert_idx.T, gates.T, w_gate, w_up, w_down)
        return out

    return jax.shard_map(device_step, mesh=mesh, in_specs=(row_spec, row_spec, row_spec, P('ep', 'fsdp', None), P('ep', 'fsdp', None), P('ep', None, 'fsdp')), out_specs=row_spec, check_vma=False)
```

```python
import functools

import jax
import jax.numpy as jnp
from jax import lax
from jax.experimental import pallas as pl
from jax.experimental.pallas import tpu as pltpu
from jax.sharding import PartitionSpec as P

MESH = pl.DeviceIdType.MESH
BF16 = jnp.bfloat16
F32 = jnp.float32

RING = 4
CHUNKS = 10
UNITS = 3
EARLY = 1
PIECES = 6


def moe_kernel(cap, tok_in, idx_ref, gates_ref, wg, wu, wd, out_ref, gu_land, d_land,
               tok, wbuf, hid, wdb, mlast, wlast, accs, in_a, in_b, in_l, in_r, gsrc, grecv, gcol, stage,
               tload, tsend, trecv, tfar, gsend, grsem,
               ysend, ssend, from_l, from_r, far_a, far_b, from_s,
               dysend, dssend, dfrom_l, dfrom_r, dfar_a, dfar_b, dfrom_s,
               lsem, dlsem, asend, asem, bsem, lsum, rsum, osem, efwd, mload):
    rows = tok_in.shape[0]
    half = rows // 2
    n_local, shard, ffn = wg.shape
    fh = ffn // 2
    hs = shard // 2
    top_k = idx_ref.shape[0]
    unit = shard // UNITS

    q = lax.axis_index('fsdp')
    ep = lax.axis_index('ep')
    chip = ep // 2
    core = ep % 2
    q_l, q_r, q_f = (q + 3) % RING, (q + 1) % RING, (q + 2) % RING
    y_r, y_l = {'fsdp': q_r}, {'fsdp': q_l}
    x_r = {'ep': ((chip + 1) % RING) * 2 + core}
    x_l = {'ep': ((chip + 3) % RING) * 2 + core}
    x_f = {'ep': ((chip + 2) % RING) * 2 + core}
    sib = {'ep': chip * 2 + 1 - core}
    mine = core * n_local
    theirs = (1 - core) * n_local

    def wait(ref, sem):
        pltpu.make_async_copy(ref, ref, sem).wait()

    def send(src, dst, ssem, rsem, dev):
        pltpu.make_async_remote_copy(src_ref=src, dst_ref=dst, send_sem=ssem, recv_sem=rsem,
                                     device_id=dev, device_id_type=MESH).start()

    def fcols(f):
        return pl.ds(pl.multiple_of(f * fh, fh), fh)

    def own_gu(n):
        e, f = n // 2, n % 2
        for dev, ssem, rsem in ((y_r, ysend, from_l), (y_l, ysend, from_r), (sib, ssend, from_s)):
            for m, w in enumerate((wg, wu)):
                send(w.at[e, :, fcols(f)], gu_land.at[mine + e, f, q, m], ssem.at[n], rsem.at[n], dev)

    def fwd_gu(n):
        e, f = n // 2, n % 2
        lref = gu_land.at[mine + e, f, q_l]
        rref = gu_land.at[mine + e, f, q_r]
        wait(lref, from_l.at[n])
        la = gu_land.at[mine + e, f, q_l, :, 0:hs, :]
        send(la, la, ysend.at[n], far_a.at[n], y_r)
        wait(rref, from_r.at[n])
        rb = gu_land.at[mine + e, f, q_r, :, hs:shard, :]
        send(rb, rb, ysend.at[n], far_b.at[n], y_l)
        send(lref, lref, ssend.at[n], from_s.at[n], sib)
        send(rref, rref, ssend.at[n], from_s.at[n], sib)

    def far_gu(n):
        e, f = n // 2, n % 2
        wait(gu_land.at[mine + e, f, q_f, :, 0:hs, :], far_a.at[n])
        wait(gu_land.at[mine + e, f, q_f, :, hs:shard, :], far_b.at[n])
        fref = gu_land.at[mine + e, f, q_f]
        send(fref, fref, ssend.at[n], from_s.at[n], sib)

    last = CHUNKS - 1
    le = last // 2
    top, low = slice(0, hs), slice(hs, shard)

    def piece_of(n, shard_id, part):
        e, f = n // 2, n % 2
        if n == last:
            return mlast.at[shard_id, part]
        return gu_land.at[mine + e, f, shard_id, :, part]

    def to_sib(n, shard_id):
        e, f = n // 2, n % 2
        src = piece_of(n, shard_id, slice(0, shard))
        dst = wlast.at[shard_id] if n == last else src
        send(src, dst, ssend.at[n], from_s.at[n], sib)

    def own_half(n):
        e, f = n // 2, n % 2

        def put(dev, part, sem, rsem):
            for m, w in enumerate((wg, wu)):
                if n == last:
                    dst = mlast.at[q, part, m * fh:(m + 1) * fh]
                else:
                    dst = gu_land.at[mine + e, f, q, m, part]
                send(w.at[e, part, f * fh:(f + 1) * fh], dst, sem, rsem, dev)

        put(y_r, top, ysend.at[n], efwd.at[last - n, 0])
        put(y_l, low, ysend.at[n], efwd.at[last - n, 1])
        put(y_r, low, ysend.at[n], from_l.at[n])
        put(y_l, top, ysend.at[n], from_r.at[n])
        if n == last:
            wait(mlast.at[q], mload)
            to_sib(n, q)
        else:
            put(sib, slice(0, shard), ssend.at[n], from_s.at[n])

    def fwd_half(n):
        la = piece_of(n, q_l, top)
        wait(la, efwd.at[last - n, 0])
        send(la, la, ysend.at[n], far_a.at[n], y_r)
        rb = piece_of(n, q_r, low)
        wait(rb, efwd.at[last - n, 1])
        send(rb, rb, ysend.at[n], far_b.at[n], y_l)

    def near_half(n):
        wait(piece_of(n, q_l, low), from_l.at[n])
        to_sib(n, q_l)
        wait(piece_of(n, q_r, top), from_r.at[n])
        to_sib(n, q_r)

    def far_half(n):
        wait(piece_of(n, q_f, top), far_a.at[n])
        wait(piece_of(n, q_f, low), far_b.at[n])
        to_sib(n, q_f)

    def own_d():
        for dev, ssem, rsem in ((y_r, dysend, dfrom_l), (y_l, dysend, dfrom_r)):
            for j in range(UNITS):
                send(wd.at[:, :, j * unit:(j + 1) * unit], d_land.at[q * UNITS + j, pl.ds(mine, n_local)],
                     ssem.at[j], rsem.at[j], dev)

    def own_d_sib():
        for j in range(UNITS):
            send(wd.at[:, :, j * unit:(j + 1) * unit], d_land.at[q * UNITS + j, pl.ds(mine, n_local)],
                 dssend.at[j], dfrom_s.at[0, j], sib)

    def fwd_d(j):
        lref = d_land.at[q_l * UNITS + j, pl.ds(mine, n_local)]
        rref = d_land.at[q_r * UNITS + j, pl.ds(mine, n_local)]
        wait(lref, dfrom_l.at[j])
        la = d_land.at[q_l * UNITS + j, pl.ds(mine, n_local), 0:fh]
        send(la, la, dysend.at[j], dfar_a.at[j], y_r)
        wait(rref, dfrom_r.at[j])
        rb = d_land.at[q_r * UNITS + j, pl.ds(mine, n_local), fh:ffn]
        send(rb, rb, dysend.at[j], dfar_b.at[j], y_l)
        send(lref, lref, dssend.at[j], dfrom_s.at[1, j], sib)
        send(rref, rref, dssend.at[j], dfrom_s.at[2, j], sib)

    def far_d(j):
        wait(d_land.at[q_f * UNITS + j, pl.ds(mine, n_local), 0:fh], dfar_a.at[j])
        wait(d_land.at[q_f * UNITS + j, pl.ds(mine, n_local), fh:ffn], dfar_b.at[j])
        fref = d_land.at[q_f * UNITS + j, pl.ds(mine, n_local)]
        send(fref, fref, dssend.at[j], dfrom_s.at[3, j], sib)

    def load_mine(n):
        e, f, par = n // 2, n % 2, n % 2
        for m, w in enumerate((wg, wu)):
            lanes = slice(m * fh, (m + 1) * fh)
            pltpu.make_async_copy(w.at[e, :, fcols(f)], wbuf.at[par, 0, q, :, lanes], lsem.at[par, 0]).start()
            for other in (q_l, q_r, q_f):
                pltpu.make_async_copy(gu_land.at[mine + e, f, other, m],
                                      wbuf.at[par, 0, other, :, lanes], lsem.at[par, 0]).start()

    def load_theirs(n, again=False):
        e, f, par = n // 2, n % 2, n % 2
        if not again:
            wait(gu_land.at[theirs + e, f], from_s.at[n])
        for m in range(2):
            pltpu.make_async_copy(gu_land.at[theirs + e, f, :, m],
                                  wbuf.at[par, 1, :, :, m * fh:(m + 1) * fh], lsem.at[par, 1]).start()

    def loaded(n, side):
        wait(wbuf.at[n % 2, side], lsem.at[n % 2, side])

    def seq_unit(s):
        if s < 3:
            return 0, s
        if s < 9:
            return (1 if s % 2 else 2), (s - 3) // 2
        return 3, s - 9

    shards = (q, q_l, q_r, q_f)

    def load_piece(p):
        for i in range(2):
            kind, j = seq_unit(2 * p + i)
            gid = shards[kind] * UNITS + j
            lanes = slice(i * unit, (i + 1) * unit)
            wait(d_land.at[gid, pl.ds(theirs, n_local)], dfrom_s.at[kind, j])
            if kind == 0:
                pltpu.make_async_copy(wd.at[:, :, j * unit:(j + 1) * unit],
                                      wdb.at[p % 2, pl.ds(mine, n_local), :, lanes], dlsem.at[p % 2]).start()
                pltpu.make_async_copy(d_land.at[gid, pl.ds(theirs, n_local)],
                                      wdb.at[p % 2, pl.ds(theirs, n_local), :, lanes], dlsem.at[p % 2]).start()
            else:
                pltpu.make_async_copy(d_land.at[gid], wdb.at[p % 2, :, :, lanes], dlsem.at[p % 2]).start()

    barrier = pltpu.get_barrier_semaphore()
    for dev in (y_r, y_l, x_r, x_l, x_f, sib):
        pl.semaphore_signal(barrier, inc=1, device_id=dev, device_id_type=MESH)
    pl.semaphore_wait(barrier, 6)

    own_gu(0)
    own_gu(1)
    own_tok = pltpu.make_async_copy(tok_in, tok.at[0], tload)
    own_tok.start()
    send(tok_in, tok.at[1], tsend.at[0], trecv.at[0], x_r)
    send(tok_in, tok.at[2], tsend.at[1], trecv.at[1], x_l)
    own_d_sib()
    for m, w in enumerate((wg, wu)):
        pltpu.make_async_copy(w.at[le, :, fh * (last % 2):fh * (last % 2 + 1)],
                              mlast.at[q, :, m * fh:(m + 1) * fh], mload).start()

    expert = lax.broadcasted_iota(jnp.int32, (128, rows), 0)
    chosen = jnp.zeros((128, rows), F32)
    gval = jnp.zeros((128, rows), F32)
    for j in range(top_k):
        hit = idx_ref[j:j + 1, :] == expert
        chosen = jnp.where(hit, 1.0, chosen)
        gval = jnp.where(hit, gates_ref[j:j + 1, :], gval)
    earlier = lax.broadcasted_iota(jnp.int32, (rows, rows), 0) < lax.broadcasted_iota(jnp.int32, (rows, rows), 1)
    before = jnp.dot(chosen.astype(BF16), jnp.where(earlier, 1.0, 0.0).astype(BF16), preferred_element_type=F32)
    gsrc[...] = jnp.where(before < cap - 0.5, gval, 0.0).T

    fwd_gu(0)
    own_gu(2)
    fwd_gu(1)
    own_gu(3)
    far_gu(0)
    load_mine(0)
    load_theirs(0)
    fwd_gu(2)
    own_gu(4)
    wait(tok.at[1], trecv.at[0])
    ta = tok.at[1, 0:half]
    send(ta, tok.at[3, 0:half], tsend.at[2], tfar.at[0], x_r)
    wait(tok.at[2], trecv.at[1])
    tb = tok.at[2, half:rows]
    send(tb, tok.at[3, half:rows], tsend.at[3], tfar.at[1], x_l)
    for i, dev in enumerate((x_r, x_l, x_f)):
        send(gsrc, grecv.at[i], gsend.at[i], grsem.at[i], dev)
    far_gu(1)
    load_mine(1)
    load_theirs(1)
    own_tok.wait()

    def gu_item(n, side, b, weights=None):
        e, f, par = n // 2, n % 2, n % 2
        w = wbuf[par, side] if weights is None else weights[...]
        both = jnp.dot(tok[b], w.reshape(RING * shard, ffn), preferred_element_type=F32)
        act_a, act_b = both[:, :fh], both[:, fh:]
        base = jnp.where(side == 0, mine, theirs)
        hid[base + e, b, :, fcols(f)] = (act_a * jax.nn.sigmoid(act_a) * act_b).astype(BF16)

    def gu_items(n, side, b0, b1):
        def body(b, carry):
            gu_item(n, side, b)
            return carry
        lax.fori_loop(b0, b1, body, 0)

    def early(n, carry):
        def side_step(side, c):
            loaded(n, side)
            gu_items(n, side, 0, 3)

            @pl.when((n == 0) & (side == 1))
            def _():
                fwd_gu(3)
                own_gu(5)

            @pl.when((n == 1) & (side == 0))
            def _():
                far_gu(2)
                load_mine(2)

            @pl.when((n == 1) & (side == 1))
            def _():
                load_theirs(2)
            return c
        lax.fori_loop(0, 2, side_step, 0)
        return carry

    lax.fori_loop(0, 3, early, 0)
    wait(tok.at[3, 0:half], tfar.at[0])
    wait(tok.at[3, half:rows], tfar.at[1])

    def late(k, carry):
        n, side = 2 - k // 2, k % 2

        @pl.when(n == 0)
        def _():
            loaded(n, side)
        gu_item(n, side, 3)

        @pl.when(k == 1)
        def _():
            load_mine(0)
            load_theirs(0, again=True)
            fwd_gu(4)
            own_gu(6)

        @pl.when(k == 4)
        def _():
            far_gu(3)
            load_mine(3)
        return carry

    lax.fori_loop(0, 6, late, 0)
    load_theirs(3)

    def steady(n, carry):
        loaded(n, 0)
        gu_items(n, 0, 0, 2)

        @pl.when(n == last - 1)
        def _():
            fwd_half(last)
            own_d()

        gu_items(n, 0, 2, 4)

        @pl.when(n == last - 2)
        def _():
            near_half(last - 1)
            load_piece(0)

        loaded(n, 1)
        gu_items(n, 1, 0, 2)

        @pl.when(n <= last - 4)
        def _():
            fwd_gu(n + 2)

            @pl.when(n == 3)
            def _():
                own_gu(7)

            @pl.when(n == last - 4)
            def _():
                own_half(last - 1)

        @pl.when(n <= last - 2)
        def _():
            far_gu(n + 1)
            load_mine(n + 1)

        gu_items(n, 1, 2, 4)

        @pl.when(n <= last - 2)
        def _():
            load_theirs(n + 1)

        @pl.when(n == last - 3)
        def _():
            fwd_half(last - 1)
            own_half(last)

        @pl.when(n == 5)
        def _():
            shift = (128 - chip * 2 * n_local) % 128
            gcol[0] = pltpu.roll(gsrc[...], shift, 1)
            for i in range(3):
                wait(grecv.at[i], grsem.at[i])
                gcol[i + 1] = pltpu.roll(grecv[i], shift, 1)
        return carry

    lax.fori_loop(3, CHUNKS - 1, steady, 0)
    near_half(last)

    def finish(p):
        s = p % 2
        wait(in_l.at[p], lsum.at[p])
        wait(in_r.at[p], rsum.at[p])
        for i in range(2):
            if isinstance(p, int):
                kind, j = seq_unit(2 * p + i)
                gid = shards[kind] * UNITS + j
            else:
                sq = 2 * p + i
                mid = sq - 3
                kind = jnp.where(sq < 3, 0, jnp.where(sq < 9, 1 + mid % 2, 3))
                j = jnp.where(sq < 3, sq, jnp.where(sq < 9, mid // 2, sq - 9))
                sh = jnp.where(kind == 0, q, jnp.where(kind == 1, q_l, jnp.where(kind == 2, q_r, q_f)))
                gid = sh * UNITS + j
            cols = pl.ds(pl.multiple_of(gid * unit, unit), unit)
            lanes = slice(i * unit, (i + 1) * unit)
            total = accs[s, 3, :, lanes] + in_l[p, :, lanes] + in_r[p, :, lanes]
            stage[:, cols] = (tok[0, :, cols].astype(F32) + total).astype(BF16)
            pltpu.make_async_copy(stage.at[:, cols], out_ref.at[:, cols], osem.at[p]).start()

    last_experts = (le, n_local + le)
    early_experts = [e for e in range(2 * n_local) if e not in last_experts]

    def combine(s, b, experts):
        gates_b = gcol[b]
        total = None
        for e in experts:
            o = jnp.dot(hid[e, b], wdb[s, e], preferred_element_type=F32).astype(BF16).astype(F32)
            g = gates_b[:, e:e + 1]
            o = jnp.where(g != 0.0, g * o, 0.0)
            total = o if total is None else total + o
        return total

    def first_part(i, carry):
        @pl.when(i == EARLY)
        def _():
            far_half(last)
        accs[0, i] = combine(0, 3 - i, early_experts)
        return carry

    wait(wdb.at[0], dlsem.at[0])
    lax.fori_loop(0, EARLY + 1, first_part, 0)

    def block_step(t, carry):
        p, i = t // 4, t % 4
        s = p % 2
        b = 3 - i

        @pl.when((i == 0) & (p > 0))
        def _():
            wait(wdb.at[s], dlsem.at[s])

        @pl.when((p >= 2) & (i < 3))
        def _():
            wait(accs.at[s, i], asend.at[p - 2, i])

        @pl.when(p == 0)
        def _():
            @pl.when(i > EARLY)
            def _():
                accs[0, i] = combine(0, b, early_experts)

            gu_item(last, 0, b, mlast)

            @pl.when(i == 0)
            def _():
                wait(wlast, from_s.at[last])
            gu_item(last, 1, b, wlast)

            @pl.when(i == 3)
            def _():
                fwd_d(0)
            accs[0, i] += combine(0, b, last_experts)

        @pl.when(p > 0)
        def _():
            accs[s, i] = combine(s, b, range(2 * n_local))

        @pl.when(i == 0)
        def _():
            send(accs.at[s, 0, 0:half], in_a.at[p], asend.at[p, 0], asem.at[p], x_r)
            send(accs.at[s, 0, half:rows], in_b.at[p], asend.at[p, 0], bsem.at[p], x_l)

            @pl.when(p == 3)
            def _():
                far_d(0)

            @pl.when(p == 4)
            def _():
                far_d(1)
                far_d(2)

        @pl.when(i == 1)
        def _():
            send(accs.at[s, 1, half:rows], in_l.at[p, half:rows], asend.at[p, 1], lsum.at[p], x_r)

        @pl.when(i == 2)
        def _():
            send(accs.at[s, 2, 0:half], in_r.at[p, 0:half], asend.at[p, 2], rsum.at[p], x_l)
            wait(in_a.at[p], asem.at[p])
            accs[s, 1, 0:half] += in_a[p]
            send(accs.at[s, 1, 0:half], in_l.at[p, 0:half], asend.at[p, 1], lsum.at[p], x_r)
            wait(in_b.at[p], bsem.at[p])
            accs[s, 2, half:rows] += in_b[p]
            send(accs.at[s, 2, half:rows], in_r.at[p, half:rows], asend.at[p, 2], rsum.at[p], x_l)

            for k in (1, 2):
                @pl.when(p == k)
                def _(k=k):
                    fwd_d(k)

        @pl.when(i == 3)
        def _():
            for k in range(1, PIECES):
                @pl.when(p == k - 1)
                def _(k=k):
                    load_piece(k)

            @pl.when(p >= 1)
            def _():
                finish(p - 1)
        return carry

    lax.fori_loop(0, 4 * PIECES, block_step, 0)
    finish(PIECES - 1)

    def drain(n, carry):
        wait(gu_land.at[0, 0, 0:3], ysend.at[n])
        wait(gu_land.at[0, 0], ssend.at[n])
        return carry

    lax.fori_loop(0, CHUNKS, drain, 0)
    for j in range(UNITS):
        wait(d_land.at[0:3, 0:n_local], dysend.at[j])
        wait(d_land.at[0:4, 0:n_local], dssend.at[j])
    wait(tok.at[1], tsend.at[0])
    wait(tok.at[1], tsend.at[1])
    wait(tok.at[1, 0:half], tsend.at[2])
    wait(tok.at[1, 0:half], tsend.at[3])
    for i in range(3):
        wait(gsrc, gsend.at[i])
    for p in (PIECES - 2, PIECES - 1):
        for i in range(3):
            wait(accs.at[0, 0], asend.at[p, i])
    for p in range(PIECES):
        wait(stage.at[:, 0:2 * unit], osem.at[p])


def solution(mesh):
    ep_size = mesh.shape['ep']
    row_spec = P(('rep', 'ep', 'fsdp'), None)

    def device_step(tokens, expert_idx, gates, w_gate, w_up, w_down):
        rows, top_k = expert_idx.shape
        n_local, shard, ffn = w_gate.shape
        model_dim = tokens.shape[1]
        num_experts = n_local * ep_size
        cap = (2 * rows * top_k + num_experts - 1) // num_experts
        fh, half, unit = ffn // 2, rows // 2, shard // UNITS
        piece = 2 * unit
        vmem = pl.BlockSpec(memory_space=pltpu.VMEM)
        hbm = pl.BlockSpec(memory_space=pl.ANY)
        dma = pltpu.SemaphoreType.DMA
        out, _, _ = pl.pallas_call(
            functools.partial(moe_kernel, cap),
            out_shape=(
                jax.ShapeDtypeStruct((rows, model_dim), BF16),
                jax.ShapeDtypeStruct((2 * n_local, 2, RING, 2, shard, fh), BF16),
                jax.ShapeDtypeStruct((RING * UNITS, 2 * n_local, ffn, unit), BF16),
            ),
            in_specs=[hbm, vmem, vmem, hbm, hbm, hbm],
            out_specs=(hbm, hbm, hbm),
            scratch_shapes=[
                pltpu.VMEM((4, rows, model_dim), BF16),
                pltpu.VMEM((2, 2, RING, shard, ffn), BF16),
                pltpu.VMEM((2 * n_local, 4, rows, ffn), BF16),
                pltpu.VMEM((2, 2 * n_local, ffn, piece), BF16),
                pltpu.VMEM((RING, shard, ffn), BF16),
                pltpu.VMEM((RING, shard, ffn), BF16),
                pltpu.VMEM((2, 4, rows, piece), F32),
                pltpu.VMEM((PIECES, half, piece), F32),
                pltpu.VMEM((PIECES, half, piece), F32),
                pltpu.VMEM((PIECES, rows, piece), F32),
                pltpu.VMEM((PIECES, rows, piece), F32),
                pltpu.VMEM((rows, 128), F32),
                pltpu.VMEM((3, rows, 128), F32),
                pltpu.VMEM((4, rows, 128), F32),
                pltpu.VMEM((rows, model_dim), BF16),
                dma, dma((4,)), dma((2,)), dma((2,)), dma((3,)), dma((3,)),
                dma((CHUNKS,)), dma((CHUNKS,)), dma((CHUNKS,)), dma((CHUNKS,)), dma((CHUNKS,)), dma((CHUNKS,)), dma((CHUNKS,)),
                dma((UNITS,)), dma((UNITS,)), dma((UNITS,)), dma((UNITS,)), dma((UNITS,)), dma((UNITS,)), dma((4, UNITS)),
                dma((2, 2)), dma((2,)), dma((PIECES, 3)), dma((PIECES,)), dma((PIECES,)), dma((PIECES,)), dma((PIECES,)), dma((PIECES,)), dma((2, 2)), dma,
            ],
            compiler_params=pltpu.CompilerParams(collective_id=0, has_side_effects=True, vmem_limit_bytes=67043328),
            name='moe_ring',
        )(tokens, expert_idx.T, gates.T, w_gate, w_up, w_down)
        return out

    return jax.shard_map(device_step, mesh=mesh, in_specs=(row_spec, row_spec, row_spec, P('ep', 'fsdp', None), P('ep', 'fsdp', None), P('ep', None, 'fsdp')), out_specs=row_spec, check_vma=False)
```

```python
import functools

import jax
import jax.numpy as jnp
from jax import lax
from jax.experimental import pallas as pl
from jax.experimental.pallas import tpu as pltpu
from jax.sharding import PartitionSpec as P

MESH = pl.DeviceIdType.MESH
BF16 = jnp.bfloat16
F32 = jnp.float32

RING = 4
CHUNKS = 10
UNITS = 3
EARLY = 1
PIECES = 6


def moe_kernel(cap, tok_in, idx_ref, gates_ref, wg, wu, wd, out_ref, gu_land, d_land,
               tok, wbuf, hid, wdb, mlast, wlast, accs, in_a, in_b, in_l, in_r, gsrc, grecv, gcol, stage,
               tload, tsend, trecv, tfar, gsend, grsem,
               ysend, ssend, from_l, from_r, far_a, far_b, from_s,
               dysend, dssend, dfrom_l, dfrom_r, dfar_a, dfar_b, dfrom_s,
               lsem, dlsem, asend, asem, bsem, lsum, rsum, osem, efwd, mload):
    rows = tok_in.shape[0]
    half = rows // 2
    n_local, shard, ffn = wg.shape
    fh = ffn // 2
    hs = shard // 2
    top_k = idx_ref.shape[0]
    unit = shard // UNITS

    q = lax.axis_index('fsdp')
    ep = lax.axis_index('ep')
    chip = ep // 2
    core = ep % 2
    q_l, q_r, q_f = (q + 3) % RING, (q + 1) % RING, (q + 2) % RING
    y_r, y_l = {'fsdp': q_r}, {'fsdp': q_l}
    x_r = {'ep': ((chip + 1) % RING) * 2 + core}
    x_l = {'ep': ((chip + 3) % RING) * 2 + core}
    x_f = {'ep': ((chip + 2) % RING) * 2 + core}
    sib = {'ep': chip * 2 + 1 - core}
    mine = core * n_local
    theirs = (1 - core) * n_local

    def wait(ref, sem):
        pltpu.make_async_copy(ref, ref, sem).wait()

    def send(src, dst, ssem, rsem, dev):
        pltpu.make_async_remote_copy(src_ref=src, dst_ref=dst, send_sem=ssem, recv_sem=rsem,
                                     device_id=dev, device_id_type=MESH).start()

    def fcols(f):
        return pl.ds(pl.multiple_of(f * fh, fh), fh)

    def own_gu(n):
        e, f = n // 2, n % 2
        for dev, ssem, rsem in ((y_r, ysend, from_l), (y_l, ysend, from_r), (sib, ssend, from_s)):
            for m, w in enumerate((wg, wu)):
                send(w.at[e, :, fcols(f)], gu_land.at[mine + e, f, q, m], ssem.at[n], rsem.at[n], dev)

    def fwd_gu(n):
        e, f = n // 2, n % 2
        lref = gu_land.at[mine + e, f, q_l]
        rref = gu_land.at[mine + e, f, q_r]
        wait(lref, from_l.at[n])
        la = gu_land.at[mine + e, f, q_l, :, 0:hs, :]
        send(la, la, ysend.at[n], far_a.at[n], y_r)
        wait(rref, from_r.at[n])
        rb = gu_land.at[mine + e, f, q_r, :, hs:shard, :]
        send(rb, rb, ysend.at[n], far_b.at[n], y_l)
        send(lref, lref, ssend.at[n], from_s.at[n], sib)
        send(rref, rref, ssend.at[n], from_s.at[n], sib)

    def far_gu(n):
        e, f = n // 2, n % 2
        wait(gu_land.at[mine + e, f, q_f, :, 0:hs, :], far_a.at[n])
        wait(gu_land.at[mine + e, f, q_f, :, hs:shard, :], far_b.at[n])
        fref = gu_land.at[mine + e, f, q_f]
        send(fref, fref, ssend.at[n], from_s.at[n], sib)

    last = CHUNKS - 1
    le = last // 2
    top, low = slice(0, hs), slice(hs, shard)

    def piece_of(n, shard_id, part):
        e, f = n // 2, n % 2
        if n == last:
            return mlast.at[shard_id, part]
        return gu_land.at[mine + e, f, shard_id, :, part]

    def to_sib(n, shard_id):
        e, f = n // 2, n % 2
        src = piece_of(n, shard_id, slice(0, shard))
        dst = wlast.at[shard_id] if n == last else src
        send(src, dst, ssend.at[n], from_s.at[n], sib)

    def own_half(n):
        e, f = n // 2, n % 2

        def put(dev, part, sem, rsem):
            for m, w in enumerate((wg, wu)):
                if n == last:
                    dst = mlast.at[q, part, m * fh:(m + 1) * fh]
                else:
                    dst = gu_land.at[mine + e, f, q, m, part]
                send(w.at[e, part, f * fh:(f + 1) * fh], dst, sem, rsem, dev)

        put(y_r, top, ysend.at[n], efwd.at[last - n, 0])
        put(y_l, low, ysend.at[n], efwd.at[last - n, 1])
        put(y_r, low, ysend.at[n], from_l.at[n])
        put(y_l, top, ysend.at[n], from_r.at[n])
        if n == last:
            wait(mlast.at[q], mload)
            to_sib(n, q)
        else:
            put(sib, slice(0, shard), ssend.at[n], from_s.at[n])

    def fwd_half(n):
        la = piece_of(n, q_l, top)
        wait(la, efwd.at[last - n, 0])
        send(la, la, ysend.at[n], far_a.at[n], y_r)
        rb = piece_of(n, q_r, low)
        wait(rb, efwd.at[last - n, 1])
        send(rb, rb, ysend.at[n], far_b.at[n], y_l)

    def near_half(n):
        wait(piece_of(n, q_l, low), from_l.at[n])
        to_sib(n, q_l)
        wait(piece_of(n, q_r, top), from_r.at[n])
        to_sib(n, q_r)

    def far_half(n):
        wait(piece_of(n, q_f, top), far_a.at[n])
        wait(piece_of(n, q_f, low), far_b.at[n])
        to_sib(n, q_f)

    def own_d():
        for dev, ssem, rsem in ((y_r, dysend, dfrom_l), (y_l, dysend, dfrom_r)):
            for j in range(UNITS):
                send(wd.at[:, :, j * unit:(j + 1) * unit], d_land.at[q * UNITS + j, pl.ds(mine, n_local)],
                     ssem.at[j], rsem.at[j], dev)

    def own_d_sib():
        for j in range(UNITS):
            send(wd.at[:, :, j * unit:(j + 1) * unit], d_land.at[q * UNITS + j, pl.ds(mine, n_local)],
                 dssend.at[j], dfrom_s.at[0, j], sib)

    def fwd_d(j):
        lref = d_land.at[q_l * UNITS + j, pl.ds(mine, n_local)]
        rref = d_land.at[q_r * UNITS + j, pl.ds(mine, n_local)]
        wait(lref, dfrom_l.at[j])
        la = d_land.at[q_l * UNITS + j, pl.ds(mine, n_local), 0:fh]
        send(la, la, dysend.at[j], dfar_a.at[j], y_r)
        wait(rref, dfrom_r.at[j])
        rb = d_land.at[q_r * UNITS + j, pl.ds(mine, n_local), fh:ffn]
        send(rb, rb, dysend.at[j], dfar_b.at[j], y_l)
        send(lref, lref, dssend.at[j], dfrom_s.at[1, j], sib)
        send(rref, rref, dssend.at[j], dfrom_s.at[2, j], sib)

    def far_d(j):
        wait(d_land.at[q_f * UNITS + j, pl.ds(mine, n_local), 0:fh], dfar_a.at[j])
        wait(d_land.at[q_f * UNITS + j, pl.ds(mine, n_local), fh:ffn], dfar_b.at[j])
        fref = d_land.at[q_f * UNITS + j, pl.ds(mine, n_local)]
        send(fref, fref, dssend.at[j], dfrom_s.at[3, j], sib)

    def load_mine(n):
        e, f, par = n // 2, n % 2, n % 2
        for m, w in enumerate((wg, wu)):
            lanes = slice(m * fh, (m + 1) * fh)
            pltpu.make_async_copy(w.at[e, :, fcols(f)], wbuf.at[par, 0, q, :, lanes], lsem.at[par, 0]).start()
            for other in (q_l, q_r, q_f):
                pltpu.make_async_copy(gu_land.at[mine + e, f, other, m],
                                      wbuf.at[par, 0, other, :, lanes], lsem.at[par, 0]).start()

    def load_theirs(n, again=False):
        e, f, par = n // 2, n % 2, n % 2
        if not again:
            wait(gu_land.at[theirs + e, f], from_s.at[n])
        for m in range(2):
            pltpu.make_async_copy(gu_land.at[theirs + e, f, :, m],
                                  wbuf.at[par, 1, :, :, m * fh:(m + 1) * fh], lsem.at[par, 1]).start()

    def loaded(n, side):
        wait(wbuf.at[n % 2, side], lsem.at[n % 2, side])

    def seq_unit(s):
        if s < 3:
            return 0, s
        if s < 9:
            return (1 if s % 2 else 2), (s - 3) // 2
        return 3, s - 9

    shards = (q, q_l, q_r, q_f)

    def load_piece(p):
        for i in range(2):
            kind, j = seq_unit(2 * p + i)
            gid = shards[kind] * UNITS + j
            lanes = slice(i * unit, (i + 1) * unit)
            wait(d_land.at[gid, pl.ds(theirs, n_local)], dfrom_s.at[kind, j])
            if kind == 0:
                pltpu.make_async_copy(wd.at[:, :, j * unit:(j + 1) * unit],
                                      wdb.at[p % 2, pl.ds(mine, n_local), :, lanes], dlsem.at[p % 2]).start()
                pltpu.make_async_copy(d_land.at[gid, pl.ds(theirs, n_local)],
                                      wdb.at[p % 2, pl.ds(theirs, n_local), :, lanes], dlsem.at[p % 2]).start()
            else:
                pltpu.make_async_copy(d_land.at[gid], wdb.at[p % 2, :, :, lanes], dlsem.at[p % 2]).start()

    barrier = pltpu.get_barrier_semaphore()
    for dev in (y_r, y_l, x_r, x_l, x_f, sib):
        pl.semaphore_signal(barrier, inc=1, device_id=dev, device_id_type=MESH)
    pl.semaphore_wait(barrier, 6)

    own_gu(0)
    own_gu(1)
    own_tok = pltpu.make_async_copy(tok_in, tok.at[0], tload)
    own_tok.start()
    send(tok_in, tok.at[1], tsend.at[0], trecv.at[0], x_r)
    send(tok_in, tok.at[2], tsend.at[1], trecv.at[1], x_l)
    own_d_sib()
    for m, w in enumerate((wg, wu)):
        pltpu.make_async_copy(w.at[le, :, fh * (last % 2):fh * (last % 2 + 1)],
                              mlast.at[q, :, m * fh:(m + 1) * fh], mload).start()

    expert = lax.broadcasted_iota(jnp.int32, (128, rows), 0)
    chosen = jnp.zeros((128, rows), F32)
    gval = jnp.zeros((128, rows), F32)
    for j in range(top_k):
        hit = idx_ref[j:j + 1, :] == expert
        chosen = jnp.where(hit, 1.0, chosen)
        gval = jnp.where(hit, gates_ref[j:j + 1, :], gval)
    earlier = lax.broadcasted_iota(jnp.int32, (rows, rows), 0) < lax.broadcasted_iota(jnp.int32, (rows, rows), 1)
    before = jnp.dot(chosen.astype(BF16), jnp.where(earlier, 1.0, 0.0).astype(BF16), preferred_element_type=F32)
    gsrc[...] = jnp.where(before < cap - 0.5, gval, 0.0).T

    fwd_gu(0)
    own_gu(2)
    fwd_gu(1)
    own_gu(3)
    far_gu(0)
    load_mine(0)
    load_theirs(0)
    fwd_gu(2)
    own_gu(4)
    wait(tok.at[1], trecv.at[0])
    ta = tok.at[1, 0:half]
    send(ta, tok.at[3, 0:half], tsend.at[2], tfar.at[0], x_r)
    wait(tok.at[2], trecv.at[1])
    tb = tok.at[2, half:rows]
    send(tb, tok.at[3, half:rows], tsend.at[3], tfar.at[1], x_l)
    for i, dev in enumerate((x_r, x_l, x_f)):
        send(gsrc, grecv.at[i], gsend.at[i], grsem.at[i], dev)
    far_gu(1)
    load_mine(1)
    load_theirs(1)
    own_tok.wait()

    def gu_item(n, side, b, weights=None):
        e, f, par = n // 2, n % 2, n % 2
        w = wbuf[par, side] if weights is None else weights[...]
        both = jnp.dot(tok[b], w.reshape(RING * shard, ffn), preferred_element_type=F32)
        act_a, act_b = both[:, :fh], both[:, fh:]
        base = jnp.where(side == 0, mine, theirs)
        hid[base + e, b, :, fcols(f)] = (act_a * jax.nn.sigmoid(act_a) * act_b).astype(BF16)

    def gu_items(n, side, b0, b1):
        def body(b, carry):
            gu_item(n, side, b)
            return carry
        lax.fori_loop(b0, b1, body, 0)

    def early(n, carry):
        def side_step(side, c):
            loaded(n, side)
            gu_items(n, side, 0, 3)

            @pl.when((n == 0) & (side == 1))
            def _():
                fwd_gu(3)
                own_gu(5)

            @pl.when((n == 1) & (side == 0))
            def _():
                far_gu(2)
                load_mine(2)

            @pl.when((n == 1) & (side == 1))
            def _():
                load_theirs(2)
            return c
        lax.fori_loop(0, 2, side_step, 0)
        return carry

    lax.fori_loop(0, 3, early, 0)
    wait(tok.at[3, 0:half], tfar.at[0])
    wait(tok.at[3, half:rows], tfar.at[1])

    def late(k, carry):
        n, side = 2 - k // 2, k % 2

        @pl.when(n == 0)
        def _():
            loaded(n, side)
        gu_item(n, side, 3)

        @pl.when(k == 1)
        def _():
            load_mine(0)
            load_theirs(0, again=True)
            fwd_gu(4)
            own_gu(6)

        @pl.when(k == 4)
        def _():
            far_gu(3)
            load_mine(3)
        return carry

    lax.fori_loop(0, 6, late, 0)
    load_theirs(3)

    def steady(n, carry):
        loaded(n, 0)
        gu_items(n, 0, 0, 2)

        @pl.when(n == last - 1)
        def _():
            fwd_half(last)
            own_d()

        gu_items(n, 0, 2, 4)

        @pl.when(n == last - 2)
        def _():
            near_half(last - 1)
            load_piece(0)

        loaded(n, 1)
        gu_items(n, 1, 0, 2)

        @pl.when(n <= last - 4)
        def _():
            fwd_gu(n + 2)

            @pl.when(n == 3)
            def _():
                own_gu(7)

            @pl.when(n == last - 4)
            def _():
                own_half(last - 1)

        @pl.when(n <= last - 2)
        def _():
            far_gu(n + 1)
            load_mine(n + 1)

        @pl.when(n == last - 3)
        def _():
            fwd_half(last - 1)
            own_half(last)

        gu_items(n, 1, 2, 4)

        @pl.when(n <= last - 2)
        def _():
            load_theirs(n + 1)

        @pl.when(n == 5)
        def _():
            shift = (128 - chip * 2 * n_local) % 128
            gcol[0] = pltpu.roll(gsrc[...], shift, 1)
            for i in range(3):
                wait(grecv.at[i], grsem.at[i])
                gcol[i + 1] = pltpu.roll(grecv[i], shift, 1)
        return carry

    lax.fori_loop(3, CHUNKS - 1, steady, 0)
    near_half(last)

    def finish(p):
        s = p % 2
        wait(in_l.at[p], lsum.at[p])
        wait(in_r.at[p], rsum.at[p])
        for i in range(2):
            if isinstance(p, int):
                kind, j = seq_unit(2 * p + i)
                gid = shards[kind] * UNITS + j
            else:
                sq = 2 * p + i
                mid = sq - 3
                kind = jnp.where(sq < 3, 0, jnp.where(sq < 9, 1 + mid % 2, 3))
                j = jnp.where(sq < 3, sq, jnp.where(sq < 9, mid // 2, sq - 9))
                sh = jnp.where(kind == 0, q, jnp.where(kind == 1, q_l, jnp.where(kind == 2, q_r, q_f)))
                gid = sh * UNITS + j
            cols = pl.ds(pl.multiple_of(gid * unit, unit), unit)
            lanes = slice(i * unit, (i + 1) * unit)
            total = accs[s, 3, :, lanes] + in_l[p, :, lanes] + in_r[p, :, lanes]
            stage[:, cols] = (tok[0, :, cols].astype(F32) + total).astype(BF16)
            pltpu.make_async_copy(stage.at[:, cols], out_ref.at[:, cols], osem.at[p]).start()

    last_experts = (le, n_local + le)
    early_experts = [e for e in range(2 * n_local) if e not in last_experts]

    def combine(s, b, experts):
        gates_b = gcol[b]
        total = None
        for e in experts:
            o = jnp.dot(hid[e, b], wdb[s, e], preferred_element_type=F32).astype(BF16).astype(F32)
            g = gates_b[:, e:e + 1]
            o = jnp.where(g != 0.0, g * o, 0.0)
            total = o if total is None else total + o
        return total

    def first_part(i, carry):
        @pl.when(i == EARLY)
        def _():
            far_half(last)
        accs[0, i] = combine(0, 3 - i, early_experts)
        return carry

    wait(wdb.at[0], dlsem.at[0])
    lax.fori_loop(0, EARLY + 1, first_part, 0)

    def block_step(t, carry):
        p, i = t // 4, t % 4
        s = p % 2
        b = 3 - i

        @pl.when((i == 0) & (p > 0))
        def _():
            wait(wdb.at[s], dlsem.at[s])

        @pl.when((p >= 2) & (i < 3))
        def _():
            wait(accs.at[s, i], asend.at[p - 2, i])

        @pl.when(p == 0)
        def _():
            @pl.when(i > EARLY)
            def _():
                accs[0, i] = combine(0, b, early_experts)

            gu_item(last, 0, b, mlast)

            @pl.when(i == 0)
            def _():
                wait(wlast, from_s.at[last])
            gu_item(last, 1, b, wlast)

            @pl.when(i == 3)
            def _():
                fwd_d(0)
            accs[0, i] += combine(0, b, last_experts)

        @pl.when(p > 0)
        def _():
            accs[s, i] = combine(s, b, range(2 * n_local))

        @pl.when(i == 0)
        def _():
            send(accs.at[s, 0, 0:half], in_a.at[p], asend.at[p, 0], asem.at[p], x_r)
            send(accs.at[s, 0, half:rows], in_b.at[p], asend.at[p, 0], bsem.at[p], x_l)

            @pl.when(p == 3)
            def _():
                far_d(0)

            @pl.when(p == 4)
            def _():
                far_d(1)
                far_d(2)

        @pl.when(i == 1)
        def _():
            send(accs.at[s, 1, half:rows], in_l.at[p, half:rows], asend.at[p, 1], lsum.at[p], x_r)

        @pl.when(i == 2)
        def _():
            send(accs.at[s, 2, 0:half], in_r.at[p, 0:half], asend.at[p, 2], rsum.at[p], x_l)
            wait(in_a.at[p], asem.at[p])
            accs[s, 1, 0:half] += in_a[p]
            send(accs.at[s, 1, 0:half], in_l.at[p, 0:half], asend.at[p, 1], lsum.at[p], x_r)
            wait(in_b.at[p], bsem.at[p])
            accs[s, 2, half:rows] += in_b[p]
            send(accs.at[s, 2, half:rows], in_r.at[p, half:rows], asend.at[p, 2], rsum.at[p], x_l)

            for k in (1, 2):
                @pl.when(p == k)
                def _(k=k):
                    fwd_d(k)

        @pl.when(i == 3)
        def _():
            for k in range(1, PIECES):
                @pl.when(p == k - 1)
                def _(k=k):
                    load_piece(k)

            @pl.when(p >= 1)
            def _():
                finish(p - 1)
        return carry

    lax.fori_loop(0, 4 * PIECES, block_step, 0)
    finish(PIECES - 1)

    def drain(n, carry):
        wait(gu_land.at[0, 0, 0:3], ysend.at[n])
        wait(gu_land.at[0, 0], ssend.at[n])
        return carry

    lax.fori_loop(0, CHUNKS, drain, 0)
    for j in range(UNITS):
        wait(d_land.at[0:3, 0:n_local], dysend.at[j])
        wait(d_land.at[0:4, 0:n_local], dssend.at[j])
    wait(tok.at[1], tsend.at[0])
    wait(tok.at[1], tsend.at[1])
    wait(tok.at[1, 0:half], tsend.at[2])
    wait(tok.at[1, 0:half], tsend.at[3])
    for i in range(3):
        wait(gsrc, gsend.at[i])
    for p in (PIECES - 2, PIECES - 1):
        for i in range(3):
            wait(accs.at[0, 0], asend.at[p, i])
    for p in range(PIECES):
        wait(stage.at[:, 0:2 * unit], osem.at[p])


def solution(mesh):
    ep_size = mesh.shape['ep']
    row_spec = P(('rep', 'ep', 'fsdp'), None)

    def device_step(tokens, expert_idx, gates, w_gate, w_up, w_down):
        rows, top_k = expert_idx.shape
        n_local, shard, ffn = w_gate.shape
        model_dim = tokens.shape[1]
        num_experts = n_local * ep_size
        cap = (2 * rows * top_k + num_experts - 1) // num_experts
        fh, half, unit = ffn // 2, rows // 2, shard // UNITS
        piece = 2 * unit
        vmem = pl.BlockSpec(memory_space=pltpu.VMEM)
        hbm = pl.BlockSpec(memory_space=pl.ANY)
        dma = pltpu.SemaphoreType.DMA
        out, _, _ = pl.pallas_call(
            functools.partial(moe_kernel, cap),
            out_shape=(
                jax.ShapeDtypeStruct((rows, model_dim), BF16),
                jax.ShapeDtypeStruct((2 * n_local, 2, RING, 2, shard, fh), BF16),
                jax.ShapeDtypeStruct((RING * UNITS, 2 * n_local, ffn, unit), BF16),
            ),
            in_specs=[hbm, vmem, vmem, hbm, hbm, hbm],
            out_specs=(hbm, hbm, hbm),
            scratch_shapes=[
                pltpu.VMEM((4, rows, model_dim), BF16),
                pltpu.VMEM((2, 2, RING, shard, ffn), BF16),
                pltpu.VMEM((2 * n_local, 4, rows, ffn), BF16),
                pltpu.VMEM((2, 2 * n_local, ffn, piece), BF16),
                pltpu.VMEM((RING, shard, ffn), BF16),
                pltpu.VMEM((RING, shard, ffn), BF16),
                pltpu.VMEM((2, 4, rows, piece), F32),
                pltpu.VMEM((PIECES, half, piece), F32),
                pltpu.VMEM((PIECES, half, piece), F32),
                pltpu.VMEM((PIECES, rows, piece), F32),
                pltpu.VMEM((PIECES, rows, piece), F32),
                pltpu.VMEM((rows, 128), F32),
                pltpu.VMEM((3, rows, 128), F32),
                pltpu.VMEM((4, rows, 128), F32),
                pltpu.VMEM((rows, model_dim), BF16),
                dma, dma((4,)), dma((2,)), dma((2,)), dma((3,)), dma((3,)),
                dma((CHUNKS,)), dma((CHUNKS,)), dma((CHUNKS,)), dma((CHUNKS,)), dma((CHUNKS,)), dma((CHUNKS,)), dma((CHUNKS,)),
                dma((UNITS,)), dma((UNITS,)), dma((UNITS,)), dma((UNITS,)), dma((UNITS,)), dma((UNITS,)), dma((4, UNITS)),
                dma((2, 2)), dma((2,)), dma((PIECES, 3)), dma((PIECES,)), dma((PIECES,)), dma((PIECES,)), dma((PIECES,)), dma((PIECES,)), dma((2, 2)), dma,
            ],
            compiler_params=pltpu.CompilerParams(collective_id=0, has_side_effects=True, vmem_limit_bytes=67043328),
            name='moe_ring',
        )(tokens, expert_idx.T, gates.T, w_gate, w_up, w_down)
        return out

    return jax.shard_map(device_step, mesh=mesh, in_specs=(row_spec, row_spec, row_spec, P('ep', 'fsdp', None), P('ep', 'fsdp', None), P('ep', None, 'fsdp')), out_specs=row_spec, check_vma=False)
```
